16 devices in a mesh: dp: 2 (over y, z), sp: 8 (over x, core).
Axes of the slice: x: 4, y: 2, z: 1, core: 2. Of those that a mesh axis runs over, the one named last changes fastest.
The devices are a block of a 4x4x8 slice.
Arguments:
- x: bfloat16 [4, 1024, 512], P('dp', 'sp'), parts along dimension 0
- w_cur: bfloat16 [12, 10, 512, 1024], replicated
- w_past: bfloat16 [12, 10, 512, 1024], replicated
- w_res: bfloat16 [12, 10, 512, 512], replicated
- w_skip: bfloat16 [12, 10, 512, 256], replicated
Outputs:
- output 1: float32 [4, 8, 128, 512], P('dp', 'sp'), parts along dimension 0
- output 2: float32 [4, 8, 128, 256], P('dp', 'sp'), parts along dimension 0
There are 2 independent parts. The reference program is written for one: setup_inputs(seed, part) draws one part's arguments, and reference() takes and returns one part's arrays. A program takes and returns all parts, laid end to end along the dimension named above; an argument that names none is the same for every part.
All inputs are finite; a program needn't handle non-finite values.
Results may differ from the reference program's by a relative error of at most 0.00889512.
Values are sent between devices in bfloat16 or wider.
A program may use at most 768 MiB of HBM per device.

```python
import jax
import jax.numpy as jnp
from jax import lax

BATCH_PART = 2
SEQ_DEV = 128
GROUP_SIZE = 8
STACKS = 12
CHANNELS = 512
SKIP_CH = 256
CYCLE_LEN = 10

SEQ_LEN = SEQ_DEV * GROUP_SIZE
LAYERS = STACKS * CYCLE_LEN


def setup_inputs(seed: int = 0, part: int = 0) -> dict:
    base_key = jax.random.key(seed)
    key_x = jax.random.fold_in(jax.random.fold_in(base_key, 1), part)
    key_w = jax.random.split(jax.random.fold_in(base_key, 2), 4)
    tap_scale = (2 * CHANNELS) ** -0.5
    out_scale = 2.0 * (CHANNELS * LAYERS) ** -0.5
    tap_shape = (STACKS, CYCLE_LEN, CHANNELS, 2 * CHANNELS)
    x = jax.random.normal(key_x, (BATCH_PART, SEQ_LEN, CHANNELS), jnp.float32)
    w_cur = jax.random.normal(key_w[0], tap_shape, jnp.float32) * tap_scale
    w_past = jax.random.normal(key_w[1], tap_shape, jnp.float32) * tap_scale
    w_res = jax.random.normal(key_w[2], (STACKS, CYCLE_LEN, CHANNELS, CHANNELS), jnp.float32) * out_scale
    w_skip = jax.random.normal(key_w[3], (STACKS, CYCLE_LEN, CHANNELS, SKIP_CH), jnp.float32) * out_scale
    return {"x": x.astype(jnp.bfloat16), "w_cur": w_cur.astype(jnp.bfloat16), "w_past": w_past.astype(jnp.bfloat16), "w_res": w_res.astype(jnp.bfloat16), "w_skip": w_skip.astype(jnp.bfloat16)}


def gated_layer(h_res, skip_acc, cur_w, past_w, res_w, skip_w, dilation):
    row_count = BATCH_PART * SEQ_LEN
    u_cur = h_res.astype(jnp.bfloat16)
    u_past = jnp.concatenate([jnp.zeros((BATCH_PART, dilation, CHANNELS), jnp.bfloat16), u_cur[:, :SEQ_LEN - dilation]], axis=1)
    pre_act = jnp.dot(u_cur.reshape(row_count, CHANNELS), cur_w, preferred_element_type=jnp.float32) + jnp.dot(u_past.reshape(row_count, CHANNELS), past_w, preferred_element_type=jnp.float32)
    gated = (jnp.tanh(pre_act[:, :CHANNELS]) * jax.nn.sigmoid(pre_act[:, CHANNELS:])).astype(jnp.bfloat16)
    h_new = h_res + jnp.dot(gated, res_w, preferred_element_type=jnp.float32).reshape(BATCH_PART, SEQ_LEN, CHANNELS)
    skip_new = skip_acc + jnp.dot(gated, skip_w, preferred_element_type=jnp.float32).reshape(BATCH_PART, SEQ_LEN, SKIP_CH)
    return h_new, skip_new


def reference(x, w_cur, w_past, w_res, w_skip):
    def stack_body(carry, weights):
        h_res, skip_acc = carry
        stack_cur, stack_past, stack_res, stack_skip = weights
        for layer_pos in range(CYCLE_LEN):
            h_res, skip_acc = gated_layer(h_res, skip_acc, stack_cur[layer_pos], stack_past[layer_pos], stack_res[layer_pos], stack_skip[layer_pos], 2 ** layer_pos)
        return (h_res, skip_acc), None

    h_start = x.astype(jnp.float32)
    skip_start = jnp.zeros((BATCH_PART, SEQ_LEN, SKIP_CH), jnp.float32)
    (h_fin, skip_fin), unused = lax.scan(stack_body, (h_start, skip_start), (w_cur, w_past, w_res, w_skip))
    h_out = h_fin.reshape(BATCH_PART, SEQ_DEV, GROUP_SIZE, CHANNELS).transpose(0, 2, 1, 3)
    skip_out = skip_fin.reshape(BATCH_PART, SEQ_DEV, GROUP_SIZE, SKIP_CH).transpose(0, 2, 1, 3)
    return (h_out, skip_out)
```

```python
import functools

import jax
import jax.numpy as jnp
from jax import lax
from jax.experimental import pallas as pl
from jax.experimental.pallas import tpu as pltpu
from jax.sharding import PartitionSpec as P

F32, BF16 = jnp.float32, jnp.bfloat16
PACK = 16
LANES = 128


def gate(z_tanh, z_sig):
    return (jnp.tanh(z_tanh) * (0.5 * jnp.tanh(0.5 * z_sig) + 0.5)).astype(BF16)


def dot(a, b):
    return jnp.dot(a, b, preferred_element_type=F32)


def kernel(cfg, x_ref, wc_ref, wp_ref, wr_ref, ws_ref, ho_ref, so_ref, wz, wo, land, u, h, sk, hst, kst, cols, w_sem, r_sem, s_sem, xs_sem, xr_sem, os_sem, or_sem):
    group_n, batch, stacks, cyc, rows, half, C, S, halo, off, per_seq = cfg
    me = lax.axis_index("sp")
    q = lax.rem(me, per_seq)
    seq = me // per_seq
    last = stacks - 1

    def load_w(s, i):
        return (
            pltpu.make_async_copy(wc_ref.at[s, i], wz.at[i, pl.ds(0, C)], w_sem.at[i, 0]),
            pltpu.make_async_copy(wp_ref.at[s, i], wz.at[i, pl.ds(C, C)], w_sem.at[i, 1]),
            pltpu.make_async_copy(wr_ref.at[s, i], wo.at[i, :, pl.ds(0, C)], w_sem.at[i, 2]),
            pltpu.make_async_copy(ws_ref.at[s, i], wo.at[i, :, pl.ds(C, S)], w_sem.at[i, 3]),
        )

    def hops(i):
        return max(1, 2**i // rows)

    def send(s, i):
        return pltpu.make_async_remote_copy(
            src_ref=u.at[i, pl.ds(rows - halo[i], halo[i])],
            dst_ref=land.at[s, pl.ds(off[i], halo[i])],
            send_sem=s_sem.at[i],
            recv_sem=r_sem.at[s, i],
            device_id={"sp": lax.rem(me + hops(i), group_n)},
            device_id_type=pl.DeviceIdType.MESH,
        )

    for i in range(cyc):
        for c in load_w(0, i):
            c.start()

    barrier = pltpu.get_barrier_semaphore()
    for k in range(1, group_n):
        pl.semaphore_signal(barrier, inc=1, device_id={"sp": lax.rem(me + k, group_n)}, device_id_type=pl.DeviceIdType.MESH)
    pl.semaphore_wait(barrier, group_n - 1)

    blocks = rows // half
    part = lax.rem(me, blocks)

    def x_remote(b):
        return pltpu.make_async_remote_copy(
            src_ref=x_ref.at[b], dst_ref=u.at[0, pl.ds(pl.multiple_of(part * half, half), half)], send_sem=xs_sem.at[b], recv_sem=xr_sem.at[part],
            device_id={"sp": b * per_seq + me // blocks}, device_id_type=pl.DeviceIdType.MESH)

    def x_local(b):
        return pltpu.make_async_copy(x_ref.at[b], u.at[0, pl.ds(pl.multiple_of(part * half, half), half)], xr_sem.at[part])

    for b in range(batch):
        @pl.when(b * per_seq + me // blocks != me)
        def _():
            x_remote(b).start()

        @pl.when(b * per_seq + me // blocks == me)
        def _():
            x_local(b).start()

    zero_slot = stacks
    land[zero_slot] = jnp.zeros(land.shape[1:], BF16)
    sk[...] = jnp.zeros(sk.shape, F32)

    for p in range(blocks):
        pltpu.make_async_copy(x_ref.at[0], u.at[0, pl.ds(p * half, half)], xr_sem.at[p]).wait()
    for b in range(batch):
        @pl.when(b * per_seq + me // blocks != me)
        def _():
            x_remote(b).wait_send()
    for p in range(blocks):
        h[pl.ds(p * half, half)] = u[0, pl.ds(p * half, half)].astype(F32)

    def past(i, slot, p):
        d = 2**i
        lo = p * half
        if d >= rows:
            return land[slot, pl.ds(off[i] + lo, half)]
        if d >= PACK:
            if lo >= d:
                return u[i, pl.ds(lo - d, half)]
            n = min(d, half)
            head = land[slot, pl.ds(off[i] + halo[i] - d + lo, n)]
            return head if n == half else jnp.concatenate([head, u[i, pl.ds(0, half - n)]], axis=0)
        head = land[slot, pl.ds(off[i] + halo[i] - PACK, PACK)] if p == 0 else u[i, pl.ds(lo - PACK, PACK)]
        both = jnp.concatenate([head.astype(F32), u[i, pl.ds(lo, half)].astype(F32)], axis=0)
        total = half + PACK
        return pltpu.roll(both, total - (PACK - d), axis=0)[:half].astype(BF16)

    H = C // 2

    def layer(s, i):
        nxt = (i + 1) % cyc
        right = q + hops(i) < per_seq
        has_left = q >= hops(i)

        @pl.when(right)
        def _():
            send(s, i).start()

        freed = (i - 1) % cyc
        if i >= 1:
            @pl.when(s < last)
            def _():
                for c in load_w(s + 1, freed):
                    c.start()
        else:
            @pl.when(s > 0)
            def _():
                for c in load_w(s, freed):
                    c.start()

        right_n = q + hops(nxt) < per_seq
        if i < cyc - 1:
            @pl.when(jnp.logical_and(right_n, s > 0))
            def _():
                send(s - 1, nxt).wait_send()
        else:
            @pl.when(right_n)
            def _():
                send(s, nxt).wait_send()

        for c in load_w(s, i):
            c.wait()

        @pl.when(has_left)
        def _():
            send(s, i).wait_recv()

        slot = jnp.where(has_left, s, zero_slot)
        parts = rows // half
        zs = []
        for p in range(parts):
            lhs = jnp.concatenate([u[i, pl.ds(p * half, half)], past(i, slot, p)], axis=1)
            zs.append([(dot(lhs, wz[i, :, pl.ds(n * H, H)]), dot(lhs, wz[i, :, pl.ds(C + n * H, H)])) for n in range(2)])
        for p in range(parts):
            r0 = pl.ds(p * half, half)
            a = jnp.concatenate([gate(*zs[p][n]) for n in range(2)], axis=1)
            new = h[r0] + dot(a, wo[i, :, pl.ds(0, C)])
            h[r0] = new
            u[nxt, r0] = new.astype(BF16)
            sk[r0] += dot(a, wo[i, :, pl.ds(C, S)])

    def stack(s, carry):
        for i in range(cyc):
            layer(s, i)
        return carry

    lax.fori_loop(0, stacks, stack, 0)

    for i in range(1, cyc):
        @pl.when(q + hops(i) < per_seq)
        def _():
            send(last, i).wait_send()

    share = rows // group_n
    for n in range(C // LANES):
        cols[n] = h[:, pl.ds(n * LANES, LANES)]
    for n in range(S // LANES):
        cols[C // LANES + n] = sk[:, pl.ds(n * LANES, LANES)]
    for j in range(group_n):
        for n in range(C // LANES):
            hst[j, :, pl.ds(n * LANES, LANES)] = cols[n, pl.ds(j, share, stride=group_n), :]
        for n in range(S // LANES):
            kst[j, :, pl.ds(n * LANES, LANES)] = cols[C // LANES + n, pl.ds(j, share, stride=group_n), :]

    def outs(j, src):
        dst = pl.ds(pl.multiple_of(q * share, share), share)
        return ((hst.at[j], ho_ref.at[seq, 0, dst]), (kst.at[j], so_ref.at[seq, 0, dst]))

    def out_remote(j, src):
        return [pltpu.make_async_remote_copy(src_ref=a, dst_ref=b, send_sem=os_sem.at[j, t], recv_sem=or_sem.at[src, t], device_id={"sp": j}, device_id_type=pl.DeviceIdType.MESH)
                for t, (a, b) in enumerate(outs(j, src))]

    for k in range(1, group_n):
        for c in out_remote(lax.rem(me + k, group_n), me):
            c.start()
    own = [pltpu.make_async_copy(a, b, or_sem.at[me, t]) for t, (a, b) in enumerate(outs(me, me))]
    for c in own:
        c.start()
    for k in range(1, group_n):
        for c in out_remote(lax.rem(me + k, group_n), me):
            c.wait_send()
        for c in out_remote(me, lax.rem(me + k, group_n)):
            c.wait_recv()
    for c in own:
        c.wait()


def solution(mesh):
    group_n = mesh.shape["sp"]

    def local_stack(x_loc, w_cur, w_past, w_res, w_skip):
        batch, half, C = x_loc.shape
        stacks, cyc, S = w_cur.shape[0], w_cur.shape[1], w_skip.shape[-1]
        per_seq = group_n // batch
        rows = half * batch
        halo = [min(max(2**i, PACK), rows) for i in range(cyc)]
        off = [sum(halo[:i]) for i in range(cyc)]
        cfg = (group_n, batch, stacks, cyc, rows, half, C, S, halo, off, per_seq)
        any_spec = pl.BlockSpec(memory_space=pl.ANY)
        return pl.pallas_call(
            functools.partial(kernel, cfg),
            out_shape=(jax.ShapeDtypeStruct((batch, 1, half, C), F32), jax.ShapeDtypeStruct((batch, 1, half, S), F32)),
            in_specs=[pl.BlockSpec(memory_space=pltpu.VMEM)] + [any_spec] * 4,
            out_specs=(any_spec, any_spec),
            scratch_shapes=[
                pltpu.VMEM((cyc, 2 * C, 2 * C), BF16),
                pltpu.VMEM((cyc, C, C + S), BF16),
                pltpu.VMEM((stacks + 1, sum(halo), C), BF16),
                pltpu.VMEM((cyc, rows, C), BF16),
                pltpu.VMEM((rows, C), F32),
                pltpu.VMEM((rows, S), F32),
                pltpu.VMEM((group_n, rows // group_n, C), F32),
                pltpu.VMEM((group_n, rows // group_n, S), F32),
                pltpu.VMEM(((C + S) // LANES, rows, LANES), F32),
                pltpu.SemaphoreType.DMA((cyc, 4)),
                pltpu.SemaphoreType.DMA((stacks, cyc)),
                pltpu.SemaphoreType.DMA((cyc,)),
                pltpu.SemaphoreType.DMA((batch,)),
                pltpu.SemaphoreType.DMA((rows // half,)),
                pltpu.SemaphoreType.DMA((group_n, 2)),
                pltpu.SemaphoreType.DMA((group_n, 2)),
            ],
            compiler_params=pltpu.CompilerParams(collective_id=0, has_side_effects=True, vmem_limit_bytes=60 * 1024 * 1024),
        )(x_loc, w_cur, w_past, w_res, w_skip)

    return jax.shard_map(local_stack, mesh=mesh, in_specs=(P("dp", "sp", None), P(), P(), P(), P()), out_specs=(P("dp", "sp", None, None), P("dp", "sp", None, None)), check_vma=False)
```
